32 devices in a mesh: groups: 2 (over y), seq: 4 (over z), head: 2 (over x), inner: 2 (over core).
Axes of the slice: x: 2, y: 2, z: 4, core: 2. Of those that a mesh axis runs over, the one named last changes fastest.
Arguments:
- queries: bfloat16 [4096, 2, 8, 128], P(('groups', 'seq'), 'head', 'inner'), parts along dimension 0, may hold values from -120 to 120
- grad_out: bfloat16 [4096, 2, 8, 128], P(('groups', 'seq'), 'head', 'inner'), parts along dimension 0, may hold values from -6 to 6
- keys: bfloat16 [4096, 2, 128], P(('groups', 'seq'), 'head'), parts along dimension 0, may hold values from -6 to 6
- values: bfloat16 [4096, 2, 128], P(('groups', 'seq'), 'head'), parts along dimension 0, may hold values from -6 to 6
- indices: int32 [2, 64, 16], P('head', 'groups'), parts along dimension 1, may hold values from 0 to 31, as said below
- valid: int32 [2, 64, 16], P('head', 'groups'), parts along dimension 1, may hold values from 0 to 1
Outputs:
- grad_queries: bfloat16 [4096, 2, 8, 128], P(('groups', 'seq'), 'head', 'inner'), parts along dimension 0
- grad_keys: bfloat16 [4096, 2, 128], P(('groups', 'seq'), 'head'), parts along dimension 0
- grad_values: bfloat16 [4096, 2, 128], P(('groups', 'seq'), 'head'), parts along dimension 0
The draws below stay inside these ranges and needn't reach their ends.
There are 2 independent parts, one for each index of `groups`. The reference program is written for one: setup_inputs(seed, part) draws one part's arguments, and reference() takes and returns one part's arrays. A program takes and returns all parts, laid end to end along the dimension named above; each array names one. Nothing has to cross between parts.
Inputs may be any that keep to these rules, and one draw needn't show every extreme that they name: `indices`: call blocks r * 8 to r * 8 + 7 run r. For every KV head and query block b: slot 0 names b and is valid; the valid slots name distinct blocks at most b; over all query blocks of run r, the valid slots name blocks of runs later than r never, and for each earlier run exactly 4 distinct blocks of it. Slots that are not valid name arbitrary blocks.
All inputs are finite; a program needn't handle non-finite values.
Results may differ from the reference program's by a relative error of at most 0.007.
Values may be sent and summed in bfloat16 or wider, within the bound.
No kernel may reach another device: no remote copies, remote signals or barrier semaphores. Data moves between devices by JAX's collectives and lax.ppermute only.
A program may use at most 64 MiB of HBM per device.

```python
import jax
import jax.numpy as jnp
from jax import lax

HD = 128
GQ = 8
KVH = 2
BLK = 64
TOPK = 16
CAP = 4
QBD = 8
NQB = 32
SEQ_LEN = 2048


def paired_fields(key):
    base = jax.random.fold_in(key, 11)
    query_key, other_key = jax.random.split(base)
    drawn_q = jnp.clip(jax.random.normal(query_key, (SEQ_LEN, KVH, GQ, HD), jnp.float32), -6.0, 6.0)
    drawn_k = jnp.clip(jax.random.normal(other_key, (SEQ_LEN, KVH, HD), jnp.float32), -6.0, 6.0)
    keys_out = drawn_k
    queries_out = drawn_q
    return (queries_out, keys_out)


def draw_queries(key, part):
    return paired_fields(key)[0].astype(jnp.bfloat16)


def draw_keys(key, part):
    return paired_fields(key)[1].astype(jnp.bfloat16)


def selection(key):
    base = jax.random.fold_in(key, 29)
    pool_key, noise_key, count_key = jax.random.split(base, 3)
    runs = NQB // QBD
    blocks = jnp.arange(NQB, dtype=jnp.int32)
    owner = blocks // QBD
    local = blocks % QBD
    pool_score = jax.random.randint(pool_key, (KVH, runs, runs, QBD), 0, 2 ** 20, jnp.int32) * QBD + jnp.arange(QBD, dtype=jnp.int32)
    order = jnp.argsort(-pool_score, axis=-1, stable=True)
    ranking = jnp.argsort(order, axis=-1, stable=True).astype(jnp.int32)
    in_pool = ranking < CAP
    pool_pair = in_pool[:, owner[:, None], owner[None, :], local[None, :]]
    pool_rank = ranking[:, owner[:, None], owner[None, :], local[None, :]]
    remote_ok = (owner[None, :] < owner[:, None])[None] & pool_pair
    own_ok = ((owner[None, :] == owner[:, None]) & (blocks[None, :] < blocks[:, None]))[None]
    is_self = (blocks[None, :] == blocks[:, None])[None]
    query_local = (blocks % QBD)[:, None][None]
    forced = remote_ok & ((owner[None, :] * CAP + pool_rank) % QBD == query_local)
    noise = jax.random.randint(noise_key, (KVH, NQB, NQB), 0, 2 ** 16, jnp.int32) * NQB + blocks
    score = noise + forced.astype(jnp.int32) * 2 ** 29 + is_self.astype(jnp.int32) * 2 ** 30
    score = jnp.where(is_self | own_ok | remote_ok, score, -1 - blocks)
    top_values, top_blocks = lax.top_k(score, TOPK)
    forced_count = jnp.sum(forced.astype(jnp.int32), axis=-1)
    drawn_count = jax.random.randint(count_key, (KVH, NQB), TOPK // 2, TOPK + 1, jnp.int32)
    keeping = jnp.maximum(drawn_count, 1 + forced_count)
    usable = (top_values >= 0) & (jnp.arange(TOPK, dtype=jnp.int32)[None, None, :] < keeping[..., None])
    return (top_blocks.astype(jnp.int32), usable.astype(jnp.int32))


def draw_indices(key, part):
    return selection(key)[0]


def draw_valid(key, part):
    return selection(key)[1]


def block_levels(rng, extent, cuts, low, high):
    loudness = 1.0
    for axis_at, blocks in cuts:
        draws = jax.random.uniform(jax.random.fold_in(jax.random.fold_in(rng, 6), axis_at), (blocks,), jnp.float32, low / len(cuts), high / len(cuts))
        loudness = loudness * jnp.repeat(jnp.exp(draws), extent[axis_at] // blocks).reshape((-1,) + (1,) * (len(extent) - 1 - axis_at))
    return loudness


def bell_draw(own_key, dims, deviation, limit, shards=(), kind=jnp.bfloat16):
    array = jax.random.normal(own_key, dims, jnp.float32) * deviation
    if len(shards) > 0:
        array = block_levels(own_key, dims, shards, -0.22, 0.18) * array
    return jnp.clip(array, min=-limit, max=limit).astype(kind)


def setup_inputs(seed: int = 0, part: int = 0) -> dict:
    arg_keys = jax.random.split(jax.random.key(seed), 7)
    part_splits = jax.random.split(jax.random.fold_in(arg_keys[6], part), 7)
    queries = draw_queries(jax.random.fold_in(jax.random.fold_in(arg_keys[6], part), 71), part)
    grad_out = bell_draw(part_splits[1], (SEQ_LEN, KVH, GQ, HD), 1.0, 6.0, ((0, 4), (1, 2), (2, 2)))
    keys = draw_keys(jax.random.fold_in(jax.random.fold_in(arg_keys[6], part), 71), part)
    values = bell_draw(part_splits[3], (SEQ_LEN, KVH, HD), 1.0, 6.0, ((0, 4), (1, 2)))
    indices = draw_indices(jax.random.fold_in(jax.random.fold_in(arg_keys[6], part), 71), part)
    valid = draw_valid(jax.random.fold_in(jax.random.fold_in(arg_keys[6], part), 71), part)
    return {"queries": queries, "grad_out": grad_out, "keys": keys, "values": values, "indices": indices, "valid": valid}


def reference(queries, grad_out, keys, values, indices, valid):
    scaling = 1.0 / jnp.sqrt(jnp.float32(HD))
    position = jnp.arange(BLK, dtype=jnp.int32)
    causal = position[None, :] <= position[:, None]

    def per_head(head):
        q_head = queries[:, head].reshape(NQB, BLK, GQ, HD)
        do_head = grad_out[:, head].reshape(NQB, BLK, GQ, HD)
        k_head = keys[:, head].reshape(NQB, BLK, HD)
        v_head = values[:, head].reshape(NQB, BLK, HD)

        def step(carry, inputs):
            key_acc, value_acc = carry
            q_block, do_block, picks, usable, block = inputs
            k_sel = k_head[picks].reshape(TOPK * BLK, HD).astype(jnp.float32)
            v_sel = v_head[picks].reshape(TOPK * BLK, HD).astype(jnp.float32)
            before = picks < block
            same = picks == block
            allowed = usable[None, :, None] & (before[None, :, None] | same[None, :, None] & causal[:, None, :])
            allowed = allowed.reshape(BLK, TOPK * BLK)[None]
            q_float = q_block.astype(jnp.float32)
            do_float = do_block.astype(jnp.float32)
            scores = jnp.einsum('igw,sw->gis', q_float, k_sel) * scaling
            highest = lax.optimization_barrier(jnp.max(jnp.where(allowed, scores, -jnp.inf), axis=-1, keepdims=True))
            weights = jnp.where(allowed, jnp.exp(scores - highest), 0.0)
            probs = weights / lax.optimization_barrier(jnp.sum(weights, axis=-1, keepdims=True))
            probs_b = probs.astype(jnp.bfloat16)
            dprobs = jnp.einsum('igw,sw->gis', do_float, v_sel)
            delta = lax.optimization_barrier(jnp.sum(probs * dprobs, axis=-1, keepdims=True))
            dscores = (probs * (dprobs - delta)).astype(jnp.bfloat16).astype(jnp.float32)
            grad_q = (jnp.einsum('gis,sw->igw', dscores, k_sel) * scaling).astype(jnp.bfloat16)
            key_terms = jnp.einsum('gis,igw->sw', dscores, q_float) * scaling
            value_terms = jnp.einsum('gis,igw->sw', probs_b.astype(jnp.float32), do_float)
            key_acc = key_acc.at[picks].add(key_terms.reshape(TOPK, BLK, HD))
            value_acc = value_acc.at[picks].add(value_terms.reshape(TOPK, BLK, HD))
            return ((key_acc, value_acc), grad_q)
        start = (jnp.zeros((NQB, BLK, HD), jnp.float32), jnp.zeros((NQB, BLK, HD), jnp.float32))
        inputs = (q_head, do_head, indices[head].astype(jnp.int32), valid[head] > 0, jnp.arange(NQB, dtype=jnp.int32))
        (key_acc, value_acc), grad_q = lax.scan(step, start, inputs)
        return (grad_q, key_acc.astype(jnp.bfloat16), value_acc.astype(jnp.bfloat16))
    grad_q, grad_k, grad_v = lax.map(per_head, jnp.arange(KVH, dtype=jnp.int32))
    grad_queries = grad_q.transpose(1, 2, 0, 3, 4).reshape(SEQ_LEN, KVH, GQ, HD)
    grad_keys = grad_k.transpose(1, 2, 0, 3).reshape(SEQ_LEN, KVH, HD)
    grad_values = grad_v.transpose(1, 2, 0, 3).reshape(SEQ_LEN, KVH, HD)
    return (grad_queries, grad_keys, grad_values)
```

```python
import functools
import math

import jax
import jax.numpy as jnp
from jax import lax
from jax.experimental import pallas as pl
from jax.experimental.pallas import tpu as pltpu
from jax.sharding import PartitionSpec as P

BLK = 64
CAP = 4
NEG = -1e30
F32 = jnp.float32
BF16 = jnp.bfloat16
NT = (((1,), (1,)), ((), ()))
TN = (((0,), (0,)), ((), ()))


def dot(a, b, dims=(((1,), (0,)), ((), ()))):
    return lax.dot_general(a, b, dims, preferred_element_type=F32)


def vmem():
    return pl.BlockSpec(memory_space=pltpu.VMEM)


def smem():
    return pl.BlockSpec(memory_space=pltpu.SMEM)


def whole(shape):
    return pl.BlockSpec(shape, lambda b: (0,) * len(shape))


def prep_kernel(idx_ref, valid_ref, k_ref, v_ref, lim_ref, send_ref, *rest, runs, here):
    packs, hit_ref = rest[:-1], rest[-1]
    seq = lax.axis_index("seq")
    inner = lax.axis_index("inner")
    slots, total = idx_ref.shape
    named = jnp.where(valid_ref[...] > 0, idx_ref[...], -1)
    block = lax.broadcasted_iota(jnp.int32, (total, total), 0)
    hit = jnp.zeros((total, total), jnp.int32)
    for t in range(slots):
        hit = jnp.where(named[t : t + 1, :] == block, 1, hit)
    hit_ref[...] = hit
    lane = lax.broadcasted_iota(jnp.int32, (here, total), 1)
    row = lax.broadcasted_iota(jnp.int32, (here, total), 0)
    lane_run = lane // here
    wide = lax.broadcasted_iota(jnp.int32, (here, 128), 1)
    tall = lax.broadcasted_iota(jnp.int32, (here, 128), 0)

    def ranks(hits, run):
        present = jnp.max(jnp.where(lane_run == run, hits, 0), axis=1, keepdims=True)
        present = jnp.broadcast_to(present, (here, 128))
        count = present
        step = 1
        while step < here:
            count = count + jnp.where(tall >= step, pltpu.roll(count, step, 0), 0)
            step *= 2
        return present, count - present

    own = hit_ref[pl.ds(pl.multiple_of(seq * here, here), here), :]
    lim_ref[0:here, 0:total] = jnp.where(own > 0, jnp.where(lane == row + seq * here, 0, BLK), -2 * BLK)
    for d in range(1, runs):
        source = jnp.maximum(seq - d, 0)
        hits = hit_ref[pl.ds(pl.multiple_of(source * here, here), here), :]
        present, rank = ranks(hits, seq)
        rank = jnp.where((present > 0) & (seq >= d), rank, -1)[:, 0:1]
        for c in range(CAP):
            picked = jnp.max(jnp.where(rank == c, hits, 0), axis=0, keepdims=True)
            at = here + (d - 1) * CAP + c
            lim_ref[at : at + 1, 0:total] = jnp.where(picked > 0, BLK, -2 * BLK)
    rows = jnp.where(inner == 0, k_ref[...].astype(F32), v_ref[...].astype(F32))
    for d in range(1, runs):
        present, rank = ranks(own, seq + d)
        place = jnp.where((present > 0) & (rank == wide), tall, 0)
        place = jnp.sum(place, axis=0, keepdims=True)
        send_ref[d - 1 : d, :] = place
        for c in range(CAP):
            which = jnp.broadcast_to(place[:, c : c + 1], (BLK, 128))
            tile = rows[0:BLK]
            for n in range(1, here):
                tile = jnp.where(which == n, rows[n * BLK : (n + 1) * BLK], tile)
            packs[d - 1][c * BLK : (c + 1) * BLK, :] = tile.astype(BF16)


def masked(s, lim_ref, first, query, diff):
    tiles = []
    for j in range(s.shape[0] // BLK):
        limit = lim_ref[first + j, query]
        tile = s[j * BLK : (j + 1) * BLK]
        keep = diff <= limit
        tiles.append(jnp.where(keep, tile, NEG))
    return jnp.concatenate(tiles, axis=0)


def key_minus_token(heads):
    shape = (BLK, BLK * heads)
    return lax.broadcasted_iota(jnp.int32, shape, 0) - lax.broadcasted_iota(jnp.int32, shape, 1) // heads


def own_stats_kernel(lim_ref, q_ref, do_ref, k_ref, v_ref, stat_ref, *, heads, here, factor):
    query = lax.axis_index("seq") * here + pl.program_id(0)
    s = dot(k_ref[...], q_ref[...], NT)
    s = masked(s, lim_ref, 0, query, key_minus_token(heads))
    top = jnp.max(s, axis=0, keepdims=True)
    w = jnp.exp2((s - top) * factor)
    dp = dot(v_ref[...], do_ref[...], NT)
    stat_ref[0, 0:1, :] = top
    stat_ref[0, 1:2, :] = jnp.sum(w, axis=0, keepdims=True)
    stat_ref[0, 2:3, :] = jnp.sum(w * dp, axis=0, keepdims=True)


def remote_kernel(lim_ref, q_ref, do_ref, stat_ref, *refs, heads, here, away, factor, scaling):
    direct, swapped = refs[:away], refs[away : 2 * away]
    ds_ref, keep_ref, send_ref, kr_ref, out_stat_ref, vr_ref, dk_ref, dv_ref = refs[2 * away :]
    step = pl.program_id(0)
    inner = lax.axis_index("inner")
    query = lax.axis_index("seq") * here + step
    span = CAP * BLK

    @pl.when(step == 0)
    def _():
        for d in range(away):
            first = jnp.where(inner == 0, direct[d][...].astype(F32), swapped[d][...].astype(F32))
            second = jnp.where(inner == 0, swapped[d][...].astype(F32), direct[d][...].astype(F32))
            kr_ref[d * span : (d + 1) * span, :] = first.astype(BF16)
            vr_ref[d * span : (d + 1) * span, :] = second.astype(BF16)
        dk_ref[...] = jnp.zeros_like(dk_ref)
        dv_ref[...] = jnp.zeros_like(dv_ref)

    q = q_ref[...]
    do = do_ref[...]
    s = dot(kr_ref[...], q, NT)
    tiles = []
    for j in range(away * CAP):
        tile = s[j * BLK : (j + 1) * BLK]
        tiles.append(jnp.where(lim_ref[here + j, query] > 0, tile, NEG))
    s = jnp.concatenate(tiles, axis=0)
    own_top = stat_ref[0, 0:1, :]
    top = jnp.maximum(own_top, jnp.max(s, axis=0, keepdims=True))
    shrink = jnp.exp2((own_top - top) * factor)
    w = jnp.exp2((s - top) * factor)
    dp = dot(vr_ref[...], do, NT)
    total = stat_ref[0, 1:2, :] * shrink + jnp.sum(w, axis=0, keepdims=True)
    delta = stat_ref[0, 2:3, :] * shrink + jnp.sum(w * dp, axis=0, keepdims=True)
    inverse = 1.0 / total
    delta = delta * inverse
    p = w * inverse
    ds = (p * (dp - delta)).astype(BF16)
    ds_ref[...] = ds
    dk_ref[...] += dot(ds, q)
    dv_ref[...] += dot(p.astype(BF16), do)
    out_stat_ref[0, 0:1, :] = top
    out_stat_ref[0, 1:2, :] = inverse
    out_stat_ref[0, 2:3, :] = delta

    @pl.when(step == pl.num_programs(0) - 1)
    def _():
        store_split(inner, dk_ref, dv_ref, keep_ref, send_ref, scaling)


def store_split(inner, dk_ref, dv_ref, keep_ref, send_ref, scaling):
    @pl.when(inner == 0)
    def _():
        keep_ref[...] = dk_ref[...] * scaling
        send_ref[...] = dv_ref[...]

    @pl.when(inner != 0)
    def _():
        keep_ref[...] = dv_ref[...]
        send_ref[...] = dk_ref[...] * scaling


def own_grads_kernel(
    lim_ref, q_ref, do_ref, k_ref, v_ref, kr_ref, ds_ref, stat_ref,
    dq_ref, keep_ref, send_ref, dk_ref, dv_ref, *, heads, here, factor, scaling,
):
    step = pl.program_id(0)
    inner = lax.axis_index("inner")
    query = lax.axis_index("seq") * here + step

    @pl.when(step == 0)
    def _():
        dk_ref[...] = jnp.zeros_like(dk_ref)
        dv_ref[...] = jnp.zeros_like(dv_ref)

    q = q_ref[...]
    do = do_ref[...]
    k = k_ref[...]
    s = dot(k, q, NT)
    s = masked(s, lim_ref, 0, query, key_minus_token(heads))
    p = jnp.exp2((s - stat_ref[0, 0:1, :]) * factor) * stat_ref[0, 1:2, :]
    dp = dot(v_ref[...], do, NT)
    ds = (p * (dp - stat_ref[0, 2:3, :])).astype(BF16)
    dk_ref[...] += dot(ds, q)
    dv_ref[...] += dot(p.astype(BF16), do)
    dq = dot(k, ds, TN) + dot(kr_ref[...], ds_ref[...], TN)
    dq_ref[...] = (dq * scaling).T.astype(BF16)

    @pl.when(step == pl.num_programs(0) - 1)
    def _():
        store_split(inner, dk_ref, dv_ref, keep_ref, send_ref, scaling)


def combine_kernel(send_ref, keep_ref, recv_ref, *refs, away):
    arrived, out_ref, acc_ref = refs[:away], refs[away], refs[away + 1]
    seq = lax.axis_index("seq")
    acc_ref[...] = keep_ref[...] + recv_ref[...]
    for d in range(1, away + 1):

        @pl.when(seq + d <= away)
        def _():
            for c in range(CAP):
                at = pl.ds(pl.multiple_of(send_ref[d - 1, c] * BLK, BLK), BLK)
                acc_ref[at, :] += arrived[d - 1][c * BLK : (c + 1) * BLK, :].astype(F32)

    out_ref[...] = acc_ref[...].astype(BF16)


def per_device(queries, grad_out, keys, values, indices, valid):
    tokens, _, heads, width = queries.shape
    runs = lax.axis_size("seq")
    away = runs - 1
    inner = lax.axis_index("inner")
    here = tokens // BLK
    total = indices.shape[1]
    scaling = 1.0 / math.sqrt(width)
    factor = scaling * math.log2(math.e)
    rows = BLK * heads
    span = CAP * BLK
    far = away * span
    lanes = -(-total // 128) * 128
    swap = [(0, 1), (1, 0)]
    q = queries.reshape(tokens * heads, width)
    do = grad_out.reshape(tokens * heads, width)
    k = keys.reshape(tokens, width)
    v = values.reshape(tokens, width)
    lim, send, *packs = pl.pallas_call(
        functools.partial(prep_kernel, runs=runs, here=here),
        in_specs=[vmem()] * 4,
        out_specs=[vmem()] * (2 + away),
        out_shape=[
            jax.ShapeDtypeStruct((here + away * CAP, lanes), jnp.int32),
            jax.ShapeDtypeStruct((away, 128), jnp.int32),
        ]
        + [jax.ShapeDtypeStruct((span, width), BF16)] * away,
        scratch_shapes=[pltpu.VMEM((total, total), jnp.int32)],
        name="prep",
    )(indices[0].T, valid[0].T, k, v)
    direct = [
        lax.ppermute(packs[d - 1], "seq", [(s, (s + d) % runs) for s in range(runs)])
        for d in range(1, runs)
    ]
    row_block = pl.BlockSpec((rows, width), lambda b: (b, 0))
    stat_block = pl.BlockSpec((1, 8, rows), lambda b: (b, 0, 0))
    stat_shape = jax.ShapeDtypeStruct((here, 8, rows), F32)
    own_stats = pl.pallas_call(
        functools.partial(own_stats_kernel, heads=heads, here=here, factor=factor),
        grid=(here,),
        in_specs=[smem(), row_block, row_block, whole((tokens, width)), whole((tokens, width))],
        out_specs=stat_block,
        out_shape=stat_shape,
        name="own_stats",
        cost_estimate=pl.CostEstimate(flops=10**9, transcendentals=10**6, bytes_accessed=10**6),
    )(lim, q, do, k, v)
    swapped = [lax.ppermute(x, "inner", swap) for x in direct]
    ds_far, keep_far, send_far, k_far, stats = pl.pallas_call(
        functools.partial(
            remote_kernel, heads=heads, here=here, away=away, factor=factor, scaling=scaling
        ),
        grid=(here,),
        in_specs=[smem(), row_block, row_block, stat_block] + [whole((span, width))] * (2 * away),
        out_specs=[
            pl.BlockSpec((far, rows), lambda b: (0, b)),
            whole((far, width)),
            whole((far, width)),
            whole((far, width)),
            stat_block,
        ],
        out_shape=[
            jax.ShapeDtypeStruct((far, tokens * heads), BF16),
            jax.ShapeDtypeStruct((far, width), F32),
            jax.ShapeDtypeStruct((far, width), F32),
            jax.ShapeDtypeStruct((far, width), BF16),
            stat_shape,
        ],
        scratch_shapes=[
            pltpu.VMEM((far, width), BF16),
            pltpu.VMEM((far, width), F32),
            pltpu.VMEM((far, width), F32),
        ],
        name="far_grads",
        cost_estimate=pl.CostEstimate(flops=2 * 10**9, transcendentals=10**6, bytes_accessed=10**6),
    )(lim, q, do, own_stats, *direct, *swapped)
    from_peer = lax.ppermute(send_far, "inner", swap)
    summed = (keep_far + from_peer).astype(BF16)
    arrived = [
        lax.ppermute(
            summed[(d - 1) * span : d * span], "seq", [(r, (r - d) % runs) for r in range(runs)]
        )
        for d in range(1, runs)
    ]
    grad_queries, keep_own, send_own = pl.pallas_call(
        functools.partial(
            own_grads_kernel, heads=heads, here=here, factor=factor, scaling=scaling
        ),
        grid=(here,),
        in_specs=[
            smem(),
            row_block,
            row_block,
            whole((tokens, width)),
            whole((tokens, width)),
            whole((far, width)),
            pl.BlockSpec((far, rows), lambda b: (0, b)),
            stat_block,
        ],
        out_specs=[row_block, whole((tokens, width)), whole((tokens, width))],
        out_shape=[
            jax.ShapeDtypeStruct((tokens * heads, width), BF16),
            jax.ShapeDtypeStruct((tokens, width), F32),
            jax.ShapeDtypeStruct((tokens, width), F32),
        ],
        scratch_shapes=[pltpu.VMEM((tokens, width), F32), pltpu.VMEM((tokens, width), F32)],
        name="own_grads",
        cost_estimate=pl.CostEstimate(flops=2 * 10**9, transcendentals=10**6, bytes_accessed=10**6),
    )(lim, q, do, k, v, k_far, ds_far, stats)
    own_peer = lax.ppermute(send_own, "inner", swap)
    mine = pl.pallas_call(
        functools.partial(combine_kernel, away=away),
        in_specs=[smem(), vmem(), vmem()] + [vmem()] * away,
        out_specs=vmem(),
        out_shape=jax.ShapeDtypeStruct((tokens, width), BF16),
        scratch_shapes=[pltpu.VMEM((tokens, width), F32)],
        name="combine",
    )(send, keep_own, own_peer, *arrived)
    other = lax.ppermute(mine, "inner", swap)
    grad_keys = jnp.where(inner == 0, mine, other).reshape(tokens, 1, width)
    grad_values = jnp.where(inner == 0, other, mine).reshape(tokens, 1, width)
    return (grad_queries.reshape(tokens, 1, heads, width), grad_keys, grad_values)


def solution(mesh):
    return jax.shard_map(
        per_device,
        mesh=mesh,
        in_specs=(
            P(("groups", "seq"), "head", "inner", None),
            P(("groups", "seq"), "head", "inner", None),
            P(("groups", "seq"), "head", None),
            P(("groups", "seq"), "head", None),
            P("head", "groups", None),
            P("head", "groups", None),
        ),
        out_specs=(
            P(("groups", "seq"), "head", "inner", None),
            P(("groups", "seq"), "head", None),
            P(("groups", "seq"), "head", None),
        ),
        check_vma=False,
    )
```
